8 devices in a mesh: dp: 1 (over z), tp: 8 (over x, y, core).
Axes of the slice: x: 2, y: 2, z: 1, core: 2. Of those that a mesh axis runs over, the one named last changes fastest.
Arguments:
- x: bfloat16 [2048, 2304], P('dp')
- dy: bfloat16 [2048, 2304], P('dp')
- gate: bfloat16 [2048, 9216], P('dp', 'tp')
- up: bfloat16 [2048, 9216], P('dp', 'tp')
- w_gate: bfloat16 [2304, 9216], P(None, 'tp')
- w_up: bfloat16 [2304, 9216], P(None, 'tp')
- w_down: bfloat16 [9216, 2304], P('tp')
Outputs:
- output 1: bfloat16 [2048, 2304], P('dp')
- output 2: bfloat16 [2304, 9216], P('dp', 'tp')
- output 3: bfloat16 [2304, 9216], P('dp', 'tp')
- output 4: bfloat16 [9216, 2304], P(('dp', 'tp'))
All inputs are finite; a program needn't handle non-finite values.
Results may differ from the reference program's by a relative error of at most 0.012.
Values are sent between devices in bfloat16 or wider.
A program may use at most 2 GiB of HBM per device.

```python
import jax
import jax.numpy as jnp

ROWS = 2048
D = 2304
FF = 9216


def act(gate, up):
    return jax.nn.gelu(gate) * up


def setup_inputs(seed: int = 0, part: int = 0) -> dict:
    kx, ky, ka, kb, kg, ku, kd = jax.random.split(jax.random.key(seed), 7)
    kx, ky, ka, kb = (jax.random.fold_in(k, part) for k in (kx, ky, ka, kb))
    drawn = {
        "x": jax.random.normal(kx, (ROWS, D), jnp.float32),
        "dy": jax.random.normal(ky, (ROWS, D), jnp.float32),
        "gate": jax.random.normal(ka, (ROWS, FF), jnp.float32),
        "up": jax.random.normal(kb, (ROWS, FF), jnp.float32),
        "w_gate": jax.random.normal(kg, (D, FF), jnp.float32) * D**-0.5,
        "w_up": jax.random.normal(ku, (D, FF), jnp.float32) * D**-0.5,
        "w_down": jax.random.normal(kd, (FF, D), jnp.float32) * FF**-0.5,
    }
    return {k: v.astype(jnp.bfloat16) for k, v in drawn.items()}


def reference(x, dy, gate, up, w_gate, w_up, w_down):
    hidden, back = jax.vjp(act, gate.astype(jnp.float32), up.astype(jnp.float32))
    d_hidden = jnp.dot(dy, w_down.T, preferred_element_type=jnp.float32)
    d_gate, d_up = (g.astype(jnp.bfloat16) for g in back(d_hidden))
    dx = jnp.dot(d_gate, w_gate.T, preferred_element_type=jnp.float32) + jnp.dot(d_up, w_up.T, preferred_element_type=jnp.float32)
    dw_gate = jnp.dot(x.T, d_gate, preferred_element_type=jnp.float32)
    dw_up = jnp.dot(x.T, d_up, preferred_element_type=jnp.float32)
    dw_down = jnp.dot(hidden.astype(jnp.bfloat16).T, dy, preferred_element_type=jnp.float32)
    return tuple(g.astype(jnp.bfloat16) for g in (dx, dw_gate, dw_up, dw_down))
```

```python
import functools

import jax
import jax.numpy as jnp
from jax import lax
from jax.experimental import pallas as pl
from jax.experimental.pallas import tpu as pltpu
from jax.sharding import PartitionSpec as P

ROWS, D, F = 2048, 2304, 1152
R = 256
H = R // 2
Q = D // 2
NK = ROWS // R
NC = 2 * NK
NT = (((1,), (1,)), ((), ()))
TN = (((0,), (0,)), ((), ()))
MESH = pl.DeviceIdType.MESH
f32, bf16 = jnp.float32, jnp.bfloat16
C1 = 0.7978845608028654
C3 = 0.044715

S_X, S_Y, S_END, DRAIN = 16, 25, 34, 6
AT = {
    2: (4, 4, 6, 6, 8, 8, 11, 11, 15, 15, 16, 16, 19, 19, 21, 21),
    3: (7, 7, 9, 9, 12, 12, 15, 15, 20, 20, 22, 22, 23, 23, 26, 26),
    4: (9, 10, 12, 13, 16, 17, 19, 20, 24, 24, 27, 27, 29, 29, 32, 32),
    5: (12, 15, 16, 18, 22, 22, 23, 23, 30, 31, 33, 34, 35, 36, 37, 38),
}


def act_back(g, u, d):
    g2 = g * g
    t = jnp.tanh(g * (C1 + (C1 * C3) * g2))
    cdf = 0.5 + 0.5 * t
    gelu = g * cdf
    slope = cdf + (0.5 * g) * (1.0 - t * t) * (C1 + (3 * C1 * C3) * g2)
    return gelu * u, d * u * slope, d * gelu


def main_kernel(
    x, dy, gate, up, wg, wu, wd,
    dx, wgu, wdo,
    gu, hid, dyv, gv, uv, xyv, term, psend, pin, r1, r2, kept1, kept2,
    ssem, rsem, wsem, isem, xsem,
):
    me = lax.axis_index("tp")
    xb, yb, cb = lax.div(me, 4), lax.rem(lax.div(me, 2), 2), lax.rem(me, 2)
    mate = me + 1 - 2 * cb

    weights = [
        pltpu.make_async_copy(wd, wdo, wsem.at[0]),
        pltpu.make_async_copy(wg, wgu.at[:, pl.ds(0, F)], wsem.at[1]),
        pltpu.make_async_copy(wu, wgu.at[:, pl.ds(F, F)], wsem.at[2]),
    ]

    def rows_in(k):
        slot = lax.rem(k, 2)
        rows = pl.ds(pl.multiple_of(k * R, R), R)
        return [
            pltpu.make_async_copy(src.at[rows], dst.at[slot], isem.at[i, slot])
            for i, (src, dst) in enumerate(((dy, dyv), (gate, gv), (up, uv)))
        ]

    def tile_in(src, j, q):
        slot = lax.rem(q, 2)
        columns = pl.ds(pl.multiple_of(j * 256, 256), 256)
        return pltpu.make_async_copy(src.at[:, columns], xyv.at[slot], xsem.at[slot])

    first = rows_in(0)
    first[0].start()
    weights[0].start()
    first[1].start()
    first[2].start()
    weights[1].start()
    weights[2].start()

    barrier = pltpu.get_barrier_semaphore()
    for other in (mate, me + 2 * (1 - 2 * yb), me + 4 * (1 - 2 * xb)):
        pl.semaphore_signal(barrier, inc=1, device_id={"tp": other}, device_id_type=MESH)
    pl.semaphore_wait(barrier, 3)

    def place(c):
        k, p = lax.div(c, 2), lax.rem(c, 2)
        b1 = xb * (1 - p) + yb * p
        b2 = yb * (1 - p) + xb * p
        n1 = me + (4 - 2 * p) * (1 - 2 * b1)
        n2 = me + (2 + 2 * p) * (1 - 2 * b2)
        return k, p, b1, b2, n1, n2

    def columns_of(p):
        return pl.ds(pl.multiple_of(p * Q, 128), Q)

    def remote(i, c, src, dst, to):
        return pltpu.make_async_remote_copy(
            src_ref=src, dst_ref=dst, send_sem=ssem.at[i, c], recv_sem=rsem.at[i, c],
            device_id={"tp": to}, device_id_type=MESH,
        )

    def sl(start, size, unit):
        return pl.ds(pl.multiple_of(start, unit), size)

    def mate_term(c):
        return remote(0, c, psend.at[lax.rem(c, 2)], pin.at[c], mate)

    def half_sum(c):
        k, p, b1, b2, n1, n2 = place(c)
        return remote(1, c, pin.at[c, sl(64 * (1 - b1), 64, 64)], r1.at[c], n1)

    def quarter_sum(c):
        k, p, b1, b2, n1, n2 = place(c)
        return remote(2, c, r1.at[c, sl(32 * (1 - b2), 32, 32)], r2.at[c], n2)

    def dx_copy(i, c, to, first_flip, second_flip, size):
        k, p, b1, b2, n1, n2 = place(c)
        r = k * R + cb * H + 64 * (b1 + first_flip * (1 - 2 * b1))
        if size == 32:
            r = r + 32 * (b2 + second_flip * (1 - 2 * b2))
        ref = dx.at[sl(r, size, 32), columns_of(p)]
        return remote(i, c, ref, ref, {"n1": n1, "n2": n2, "mate": mate}[to])

    def final(c, to):
        return dx_copy({"n2": 3, "n1": 4, "mate": 6}[to], c, to, 0, 0, 32)

    def forward(c, to):
        return dx_copy({"n1": 5, "mate": 7}[to], c, to, 0, 1, 32)

    def last(c):
        return dx_copy(8, c, "mate", 1, 0, 64)

    def blocks(n, body):
        lax.fori_loop(0, n, lambda i, z: (body(i), z)[1], 0)

    def stage0(k):
        for p in range(2):
            c = 2 * k + p

            @pl.when(k > 0)
            def _():
                mate_term(c - 2).wait_send()

            def body(i):
                rows = sl(H * (1 - cb) + 16 * i, 16, 16)
                psend[p, sl(16 * i, 16, 16), :] = term[rows, p * Q:(p + 1) * Q].astype(bf16)

            blocks(H // 16, body)
            mate_term(c).start()

    def stage1(c):
        k, p, b1, b2, n1, n2 = place(c)
        mate_term(c).wait_recv()
        cols = columns_of(p)

        def total(r):
            return term[sl(H * cb + r, 16, 16), cols] + pin[c, sl(r, 16, 16), :].astype(f32)

        def out(i):
            r = 64 * (1 - b1) + 16 * i
            pin[c, sl(r, 16, 16), :] = total(r).astype(bf16)

        def keep(i):
            kept1[lax.rem(c, 8), sl(16 * i, 16, 16), :] = total(64 * b1 + 16 * i)

        blocks(4, out)
        half_sum(c).start()
        blocks(4, keep)

    def stage2(c):
        k, p, b1, b2, n1, n2 = place(c)
        half_sum(c).wait_recv()

        def total(r):
            return kept1[lax.rem(c, 8), sl(r, 16, 16), :] + r1[c, sl(r, 16, 16), :].astype(f32)

        def out(i):
            r = 32 * (1 - b2) + 16 * i
            r1[c, sl(r, 16, 16), :] = total(r).astype(bf16)

        def keep(i):
            kept2[c, sl(16 * i, 16, 16), :] = total(32 * b2 + 16 * i)

        blocks(2, out)
        quarter_sum(c).start()
        blocks(2, keep)

    def stage3(c):
        k, p, b1, b2, n1, n2 = place(c)
        quarter_sum(c).wait_recv()
        base = k * R + cb * H + 64 * b1 + 32 * b2
        cols = columns_of(p)

        def body(i):
            t = kept2[c, sl(16 * i, 16, 16), :] + r2[c, sl(16 * i, 16, 16), :].astype(f32)
            dx[sl(base + 16 * i, 16, 16), cols] = t.astype(bf16)

        blocks(2, body)
        for to in ("n2", "n1", "mate"):
            final(c, to).start()

    def stage4(c):
        final(c, "n2").wait_recv()
        for to in ("n1", "mate"):
            forward(c, to).start()

    def stage5(c):
        final(c, "n1").wait_recv()
        forward(c, "n1").wait_recv()
        last(c).start()

    def count(stage, s):
        n = jnp.int32(0)
        for at in AT[stage]:
            n = n + jnp.where(s >= at, 1, 0)
        return n

    def serve(s):
        for stage, run in ((5, stage5), (4, stage4), (3, stage3), (2, stage2)):
            lax.fori_loop(
                count(stage, s - 1), count(stage, s), lambda c, z: (run(c), z)[1], 0
            )

    def chunk(k, z):
        slot = lax.rem(k, 2)

        @pl.when(k + 1 < NK)
        def _():
            for copy in rows_in(k + 1):
                copy.start()

        for copy in rows_in(k):
            copy.wait()

        @pl.when(k == 0)
        def _():
            weights[0].wait()

        rows = sl(k * R, R, R)
        for n0, n1 in ((0, 256), (256, 512), (512, 768), (768, 1024), (1024, 1152)):
            d = lax.dot_general(dyv[slot], wdo[n0:n1, :], NT, preferred_element_type=f32)
            h, dg, du = act_back(
                gv[slot, :, n0:n1].astype(f32), uv[slot, :, n0:n1].astype(f32), d
            )
            gu[rows, n0:n1] = dg.astype(bf16)
            gu[rows, F + n0:F + n1] = du.astype(bf16)
            hid[rows, n0:n1] = h.astype(bf16)

        @pl.when(k == 0)
        def _():
            weights[1].wait()
            weights[2].wait()

        @pl.when(k > 0)
        def _():
            stage1(2 * k - 2)
            stage1(2 * k - 1)

        serve(2 * k)
        for n0 in range(0, D, 768):
            term[:, n0:n0 + 768] = lax.dot_general(
                gu[rows, :], wgu[n0:n0 + 768, :], NT, preferred_element_type=f32
            )
        stage0(k)
        serve(2 * k + 1)
        return z

    lax.fori_loop(0, NK, chunk, 0)
    tile_in(x, 0, 0).start()
    lax.fori_loop(2 * NK - 2, 2 * NK, lambda c, z: (stage1(c), z)[1], 0)

    def x_tile(j, z):
        slot = lax.rem(j, 2)

        @pl.when(j + 1 < 9)
        def _():
            tile_in(x, j + 1, j + 1).start()

        @pl.when(j + 1 == 9)
        def _():
            tile_in(dy, 0, 9).start()

        tile_in(x, j, j).wait()
        rows = sl(j * 256, 256, 256)
        for n0 in range(0, D, 768):
            wgu[rows, n0:n0 + 768] = lax.dot_general(
                xyv[slot], gu[:, n0:n0 + 768], TN, preferred_element_type=f32
            ).astype(bf16)
        serve(S_X + j)
        return z

    lax.fori_loop(0, 9, x_tile, 0)

    def y_tile(j, z):
        slot = lax.rem(j + 1, 2)

        @pl.when(j + 1 < 9)
        def _():
            tile_in(dy, j + 1, j + 10).start()

        tile_in(dy, j, j + 9).wait()
        wdo[:, sl(j * 256, 256, 256)] = lax.dot_general(
            hid[...], xyv[slot], TN, preferred_element_type=f32
        ).astype(bf16)
        serve(S_Y + j)
        return z

    lax.fori_loop(0, 9, y_tile, 0)
    lax.fori_loop(S_END, S_END + DRAIN, lambda s, z: (serve(s), z)[1], 0)

    def finish(c, z):
        @pl.when(c >= NC - 2)
        def _():
            mate_term(c).wait_send()

        half_sum(c).wait_send()
        quarter_sum(c).wait_send()
        for to in ("n2", "n1", "mate"):
            final(c, to).wait_send()
        for to in ("n1", "mate"):
            forward(c, to).wait_send()
        last(c).wait_send()
        final(c, "mate").wait_recv()
        forward(c, "mate").wait_recv()
        last(c).wait_recv()
        return z

    lax.fori_loop(0, NC, finish, 0)


def write_kernel(dx, wgu, wdo, dx_o, wg_o, wu_o, wd_o, sem):
    copies = [
        pltpu.make_async_copy(dx, dx_o, sem.at[0]),
        pltpu.make_async_copy(wgu.at[:, pl.ds(0, F)], wg_o, sem.at[1]),
        pltpu.make_async_copy(wgu.at[:, pl.ds(F, F)], wu_o, sem.at[2]),
        pltpu.make_async_copy(wdo, wd_o, sem.at[3]),
    ]
    for copy in copies:
        copy.start()
    for copy in copies:
        copy.wait()


def solution(mesh):
    hbm = pl.BlockSpec(memory_space=pltpu.HBM)
    vmem = pl.BlockSpec(memory_space=pltpu.VMEM)

    def step(x, dy, gate, up, wg, wu, wd):
        dx, wgu, wdo = pl.pallas_call(
            main_kernel,
            name="mlp_back",
            out_shape=(
                pltpu.VMEM((ROWS, D), bf16),
                pltpu.VMEM((D, D), bf16),
                pltpu.VMEM((F, D), bf16),
            ),
            in_specs=[hbm] * 7,
            out_specs=(vmem,) * 3,
            scratch_shapes=[
                pltpu.VMEM((ROWS, D), bf16),
                pltpu.VMEM((ROWS, F), bf16),
                pltpu.VMEM((2, R, D), bf16),
                pltpu.VMEM((2, R, F), bf16),
                pltpu.VMEM((2, R, F), bf16),
                pltpu.VMEM((2, ROWS, 256), bf16),
                pltpu.VMEM((R, D), f32),
                pltpu.VMEM((2, H, Q), bf16),
                pltpu.VMEM((NC, H, Q), bf16),
                pltpu.VMEM((NC, 64, Q), bf16),
                pltpu.VMEM((NC, 32, Q), bf16),
                pltpu.VMEM((8, 64, Q), f32),
                pltpu.VMEM((NC, 32, Q), f32),
                pltpu.SemaphoreType.DMA((9, NC)),
                pltpu.SemaphoreType.DMA((9, NC)),
                pltpu.SemaphoreType.DMA((3,)),
                pltpu.SemaphoreType.DMA((3, 2)),
                pltpu.SemaphoreType.DMA((2,)),
            ],
            compiler_params=pltpu.CompilerParams(
                collective_id=0, has_side_effects=True, vmem_limit_bytes=39 * 2**20
            ),
            cost_estimate=pl.CostEstimate(
                flops=12 * ROWS * D * F, bytes_accessed=80 * 2**20, transcendentals=ROWS * F
            ),
        )(x, dy, gate, up, wg, wu, wd)
        return pl.pallas_call(
            write_kernel,
            name="write_out",
            out_shape=(
                jax.ShapeDtypeStruct((ROWS, D), bf16),
                jax.ShapeDtypeStruct((D, F), bf16),
                jax.ShapeDtypeStruct((D, F), bf16),
                jax.ShapeDtypeStruct((F, D), bf16),
            ),
            in_specs=[vmem] * 3,
            out_specs=(hbm,) * 4,
            scratch_shapes=[pltpu.SemaphoreType.DMA((4,))],
            compiler_params=pltpu.CompilerParams(vmem_limit_bytes=8 * 2**20),
        )(dx, wgu, wdo)

    tokens, columns, rows = P("dp", None), P(None, "tp"), P("tp", None)
    return jax.shard_map(
        step,
        mesh=mesh,
        in_specs=(tokens, tokens, P("dp", "tp"), P("dp", "tp"), columns, columns, rows),
        out_specs=(tokens, P("dp", "tp"), P("dp", "tp"), P(("dp", "tp"), None)),
        check_vma=False,
    )
```

```python
import functools

import jax
import jax.numpy as jnp
from jax import lax
from jax.experimental import pallas as pl
from jax.experimental.pallas import tpu as pltpu
from jax.sharding import PartitionSpec as P

ROWS, D, F = 2048, 2304, 1152
R = 256
H = R // 2
Q = D // 2
NK = ROWS // R
NT = (((1,), (1,)), ((), ()))
TN = (((0,), (0,)), ((), ()))
MESH = pl.DeviceIdType.MESH
f32, bf16 = jnp.float32, jnp.bfloat16
C1 = 0.7978845608028654
C3 = 0.044715

S_X, S_Y, S_END = 14, 23, 32
AT = {
    2: (3, 4, 6, 9, 11, 13, 17, 19),
    3: (5, 7, 10, 13, 15, 19, 21, 23),
    4: (8, 14, 21, 21, 22, 25, 27, 29),
    5: (17, 19, 27, 29, 30, 32, 33, 34),
}
EARLY, EARLY_CHUNKS = 33, 6
D_TILES = ((0, 256), (256, 512), (512, 768), (768, 1024), (1024, 1152))


def act_back(g, u, d):
    g2 = g * g
    t = jnp.tanh(g * (C1 + (C1 * C3) * g2))
    cdf = 0.5 + 0.5 * t
    gelu = g * cdf
    slope = cdf + (0.5 * g) * (1.0 - t * t) * (C1 + (3 * C1 * C3) * g2)
    return gelu * u, d * u * slope, d * gelu


def main_kernel(
    x, dy, gate, up, wg, wu, wd,
    dx, wgu, wdo,
    gu, hid, cur0, cur1, dyv, gv, uv, xyv, own, psend, pin, r1, r2, kept1, kept2,
    ssem, rsem, wsem, isem, xsem,
):
    me = lax.axis_index("tp")
    xb, yb, cb = lax.div(me, 4), lax.rem(lax.div(me, 2), 2), lax.rem(me, 2)
    mate = me + 1 - 2 * cb

    def wd_in(i):
        rows = pl.ds((0, 512)[i], (512, 640)[i])
        return pltpu.make_async_copy(wd.at[rows], wdo.at[rows], wsem.at[0, i])

    def wgu_in(i):
        rows = pl.ds(768 * i, 768)
        return [
            pltpu.make_async_copy(w.at[rows], wgu.at[rows, pl.ds(F * q, F)], wsem.at[1 + q, i])
            for q, w in enumerate((wg, wu))
        ]

    def half_rows(k, half):
        at = k * R + H * (half * cb + (1 - half) * (1 - cb))
        return pl.ds(pl.multiple_of(at, H), H)

    def rows_in(k):
        slot = lax.rem(k, 2)
        return [
            pltpu.make_async_copy(
                src.at[half_rows(k, half)],
                dst.at[slot, pl.ds(H * half, H)],
                isem.at[i, half, slot],
            )
            for i, (src, dst) in enumerate(((dy, dyv), (gate, gv), (up, uv)))
            for half in range(2)
        ]

    def tile_in(src, j, q):
        slot = lax.rem(q, 2)
        columns = pl.ds(pl.multiple_of(j * 256, 256), 256)
        return pltpu.make_async_copy(src.at[:, columns], xyv.at[slot], xsem.at[slot])

    for copy in rows_in(0):
        copy.start()
    for i in range(2):
        wd_in(i).start()

    barrier = pltpu.get_barrier_semaphore()
    for other in (mate, me + 2 * (1 - 2 * yb), me + 4 * (1 - 2 * xb)):
        pl.semaphore_signal(barrier, inc=1, device_id={"tp": other}, device_id_type=MESH)

    x_pair, y_pair = (xb, me + 4 * (1 - 2 * xb)), (yb, me + 2 * (1 - 2 * yb))
    LINKS = ((x_pair, y_pair), (y_pair, x_pair))

    def remote(i, k, p, src, dst, to):
        return pltpu.make_async_remote_copy(
            src_ref=src, dst_ref=dst, send_sem=ssem.at[i, p, k], recv_sem=rsem.at[i, p, k],
            device_id={"tp": to}, device_id_type=MESH,
        )

    def sl(start, size, unit):
        return pl.ds(pl.multiple_of(start, unit), size)

    keep1, give1, keep2, give2 = ([f(p) for p in range(2)] for f in (
        lambda p: 64 * LINKS[p][0][0],
        lambda p: 64 - 64 * LINKS[p][0][0],
        lambda p: 32 * LINKS[p][1][0],
        lambda p: 32 - 32 * LINKS[p][1][0],
    ))

    def mate_term(k, p):
        return remote(0, k, p, psend.at[p], pin.at[p, k], mate)

    def half_sum(k, p):
        return remote(1, k, p, pin.at[p, k, sl(give1[p], 64, 64)], r1.at[p, k], LINKS[p][0][1])

    def quarter_sum(k, p):
        return remote(2, k, p, r1.at[p, k, sl(give2[p], 32, 32)], r2.at[p, k], LINKS[p][1][1])

    def dx_copy(i, k, p, to, row, size):
        ref = dx.at[sl(k * R + (cb * H + row), size, 32), p * Q:(p + 1) * Q]
        return remote(i, k, p, ref, ref, to)

    def final(k, p, to):
        i, device = {
            "second": (3, LINKS[p][1][1]), "first": (4, LINKS[p][0][1]), "mate": (6, mate)
        }[to]
        return dx_copy(i, k, p, device, keep1[p] + keep2[p], 32)

    def forward(k, p, to):
        i, device = {"first": (5, LINKS[p][0][1]), "mate": (7, mate)}[to]
        return dx_copy(i, k, p, device, keep1[p] + give2[p], 32)

    def last(k, p):
        return dx_copy(8, k, p, mate, give1[p], 64)

    def ring(k):
        return lax.rem(k, 4)

    def stage1(k, p):
        mate_term(k, p).wait_recv()

        def total(r):
            mine = own[sl(r, 16, 16), p * Q:(p + 1) * Q]
            return mine + pin[p, k, sl(r, 16, 16), :].astype(f32)

        for i in range(4):
            r = give1[p] + 16 * i
            pin[p, k, sl(r, 16, 16), :] = total(r).astype(bf16)
        half_sum(k, p).start()
        for i in range(4):
            kept1[p, ring(k), 16 * i:16 * i + 16, :] = total(keep1[p] + 16 * i)

    def stage2(k, p):
        half_sum(k, p).wait_recv()

        def total(r):
            mine = kept1[p, ring(k), sl(r, 16, 16), :]
            return mine + r1[p, k, sl(r, 16, 16), :].astype(f32)

        for i in range(2):
            r = give2[p] + 16 * i
            r1[p, k, sl(r, 16, 16), :] = total(r).astype(bf16)
        quarter_sum(k, p).start()
        for i in range(2):
            kept2[p, ring(k), 16 * i:16 * i + 16, :] = total(keep2[p] + 16 * i)

    def stage3(k, p):
        quarter_sum(k, p).wait_recv()
        base = k * R + (cb * H + keep1[p] + keep2[p])
        for i in range(2):
            part = slice(16 * i, 16 * i + 16)
            t = kept2[p, ring(k), part, :] + r2[p, k, part, :].astype(f32)
            dx[sl(base + 16 * i, 16, 16), p * Q:(p + 1) * Q] = t.astype(bf16)
        for to in ("second", "first", "mate"):
            final(k, p, to).start()

    def stage4(k, p):
        final(k, p, "second").wait_recv()
        for to in ("first", "mate"):
            forward(k, p, to).start()

    def stage5(k, p):
        final(k, p, "first").wait_recv()
        forward(k, p, "first").wait_recv()
        last(k, p).start()

    STAGES = {2: stage2, 3: stage3, 4: stage4, 5: stage5}

    def run_step(step):
        for stage in (5, 4, 3, 2):
            for k in range(NK):
                if AT[stage][k] == step:
                    STAGES[stage](k, 0)
                    STAGES[stage](k, 1)

    def serve(i, first, stride, turns):
        for v in range(turns):
            if any(first + stride * v in at for at in AT.values()):
                pl.when(i == v)(functools.partial(run_step, first + stride * v))

    def back_tile(k, cur, n0, n1):
        slot = lax.rem(k, 2)
        d = lax.dot_general(dyv[slot], wdo[n0:n1, :], NT, preferred_element_type=f32)
        grads = act_back(gv[slot, :, n0:n1].astype(f32), uv[slot, :, n0:n1].astype(f32), d)
        h, dg, du = (g.astype(bf16) for g in grads)
        cur[:, n0:n1] = dg
        cur[:, F + n0:F + n1] = du
        for half in range(2):
            rows, part = half_rows(k, half), slice(H * half, H * half + H)
            gu[rows, n0:n1] = dg[part]
            gu[rows, F + n0:F + n1] = du[part]
            hid[rows, n0:n1] = h[part]

    def term_tile(cur, n0):
        t = lax.dot_general(
            cur[...], wgu[n0:n0 + 768, :], NT, preferred_element_type=f32
        )
        own[:, n0:n0 + 768] = t[H:]
        for p, q0, q1 in ((0, n0, min(n0 + 768, Q)), (1, max(n0, Q), n0 + 768)):
            if q0 < q1:
                psend[p, :, q0 - p * Q:q1 - p * Q] = t[:H, q0 - n0:q1 - n0].astype(bf16)

    def send_term(k):
        for p in range(2):
            mate_term(k, p).start()

    def chunk_sum(k):
        stage1(k, 0)
        stage1(k, 1)

    def chunk_step(m, k, first, cur, ahead, start_rows):
        for p in range(2):
            mate_term(k - 1, p).wait_send()
        for copy in rows_in(k + 1):
            copy.wait()
        start_rows()
        for n0 in range(0, D, 768):
            term_tile(cur, n0)
        send_term(k)
        serve(m, first, 4, 3)
        for n0, n1 in D_TILES:
            back_tile(k + 1, ahead, n0, n1)
        chunk_sum(k)
        serve(m, first + 1, 4, 3)

    for copy in rows_in(0):
        copy.wait()
    for i in range(3):
        for copy in wgu_in(i):
            copy.start()
    wd_in(0).wait()
    for n0, n1 in D_TILES:
        if n0 == 512:
            wd_in(1).wait()
        back_tile(0, cur0, n0, n1)
    for copy in rows_in(1):
        copy.start()
    for i in range(3):
        for copy in wgu_in(i):
            copy.wait()
        term_tile(cur0, 768 * i)
    pl.semaphore_wait(barrier, 3)
    send_term(0)
    for copy in rows_in(1):
        copy.wait()
    for copy in rows_in(2):
        copy.start()
    for n0, n1 in D_TILES:
        back_tile(1, cur1, n0, n1)
    chunk_sum(0)

    def two_chunks(m, z):
        def next_rows(k):
            for copy in rows_in(k):
                copy.start()

        chunk_step(m, 2 * m + 1, 1, cur1, cur0, lambda: next_rows(2 * m + 3))
        chunk_step(
            m, 2 * m + 2, 3, cur0, cur1,
            lambda: pl.when(m < 2)(lambda: next_rows(2 * m + 4)),
        )
        return z

    lax.fori_loop(0, NK // 2 - 1, two_chunks, 0)
    tile_in(x, 0, 0).start()
    for p in range(2):
        mate_term(NK - 2, p).wait_send()
    for n0 in range(0, D, 768):
        term_tile(cur1, n0)
    send_term(NK - 1)
    run_step(2 * NK - 3)

    def x_tile(j, z):
        slot = lax.rem(j, 2)

        @pl.when(j + 1 < 9)
        def _():
            tile_in(x, j + 1, j + 1).start()

        @pl.when(j + 1 == 9)
        def _():
            tile_in(dy, 0, 9).start()

        tile_in(x, j, j).wait()
        rows = sl(j * 256, 256, 256)
        for n0 in range(0, D, 768):
            wgu[rows, n0:n0 + 768] = lax.dot_general(
                xyv[slot], gu[:, n0:n0 + 768], TN, preferred_element_type=f32
            ).astype(bf16)

        @pl.when(j == 0)
        def _():
            chunk_sum(NK - 1)

        serve(j, S_X, 1, 9)
        return z

    lax.fori_loop(0, 9, x_tile, 0)

    def y_tile(j, z):
        slot = lax.rem(j + 1, 2)

        @pl.when(j + 1 < 9)
        def _():
            tile_in(dy, j + 1, j + 10).start()

        tile_in(dy, j, j + 9).wait()
        wdo[:, sl(j * 256, 256, 256)] = lax.dot_general(
            hid[...], xyv[slot], TN, preferred_element_type=f32
        ).astype(bf16)
        serve(j, S_Y, 1, 9)
        return z

    lax.fori_loop(0, 9, y_tile, 0)
    def finish(k):
        for p in range(2):
            half_sum(k, p).wait_send()
            quarter_sum(k, p).wait_send()
            for to in ("second", "first", "mate"):
                final(k, p, to).wait_send()
            for to in ("first", "mate"):
                forward(k, p, to).wait_send()
            last(k, p).wait_send()
            final(k, p, "mate").wait_recv()
            forward(k, p, "mate").wait_recv()
            last(k, p).wait_recv()

    for p in range(2):
        mate_term(NK - 1, p).wait_send()
    for step in range(S_END, max(AT[5]) + 1):
        run_step(step)
        if step == EARLY:
            for k in range(EARLY_CHUNKS):
                finish(k)
    for k in range(EARLY_CHUNKS, NK):
        finish(k)


def write_kernel(dx, wgu, wdo, dx_o, wg_o, wu_o, wd_o, sem):
    copies = [
        pltpu.make_async_copy(dx, dx_o, sem.at[0]),
        pltpu.make_async_copy(wgu.at[:, pl.ds(0, F)], wg_o, sem.at[1]),
        pltpu.make_async_copy(wgu.at[:, pl.ds(F, F)], wu_o, sem.at[2]),
        pltpu.make_async_copy(wdo, wd_o, sem.at[3]),
    ]
    for copy in copies:
        copy.start()
    for copy in copies:
        copy.wait()


def solution(mesh):
    hbm = pl.BlockSpec(memory_space=pltpu.HBM)
    vmem = pl.BlockSpec(memory_space=pltpu.VMEM)

    def step(x, dy, gate, up, wg, wu, wd):
        results = pl.pallas_call(
            main_kernel,
            name="mlp_back",
            out_shape=(
                pltpu.VMEM((ROWS, D), bf16),
                pltpu.VMEM((D, D), bf16),
                pltpu.VMEM((F, D), bf16),
            ),
            in_specs=[hbm] * 7,
            out_specs=(vmem,) * 3,
            scratch_shapes=[
                pltpu.VMEM((ROWS, D), bf16),
                pltpu.VMEM((ROWS, F), bf16),
                pltpu.VMEM((R, D), bf16),
                pltpu.VMEM((R, D), bf16),
                pltpu.VMEM((2, R, D), bf16),
                pltpu.VMEM((2, R, F), bf16),
                pltpu.VMEM((2, R, F), bf16),
                pltpu.VMEM((2, ROWS, 256), bf16),
                pltpu.VMEM((H, D), f32),
                pltpu.VMEM((2, H, Q), bf16),
                pltpu.VMEM((2, NK, H, Q), bf16),
                pltpu.VMEM((2, NK, 64, Q), bf16),
                pltpu.VMEM((2, NK, 32, Q), bf16),
                pltpu.VMEM((2, 4, 64, Q), f32),
                pltpu.VMEM((2, 4, 32, Q), f32),
                pltpu.SemaphoreType.DMA((9, 2, NK)),
                pltpu.SemaphoreType.DMA((9, 2, NK)),
                pltpu.SemaphoreType.DMA((3, 3)),
                pltpu.SemaphoreType.DMA((3, 2, 2)),
                pltpu.SemaphoreType.DMA((2,)),
            ],
            compiler_params=pltpu.CompilerParams(
                collective_id=0, has_side_effects=True, vmem_limit_bytes=38 * 2**20
            ),
            cost_estimate=pl.CostEstimate(
                flops=12 * ROWS * D * F, bytes_accessed=80 * 2**20, transcendentals=ROWS * F
            ),
        )(x, dy, gate, up, wg, wu, wd)
        return pl.pallas_call(
            write_kernel,
            name="write_out",
            out_shape=(
                jax.ShapeDtypeStruct((ROWS, D), bf16),
                jax.ShapeDtypeStruct((D, F), bf16),
                jax.ShapeDtypeStruct((D, F), bf16),
                jax.ShapeDtypeStruct((F, D), bf16),
            ),
            in_specs=[vmem] * 3,
            out_specs=(hbm,) * 4,
            scratch_shapes=[pltpu.SemaphoreType.DMA((4,))],
            compiler_params=pltpu.CompilerParams(vmem_limit_bytes=8 * 2**20),
        )(*results)

    tokens, columns, rows = P("dp", None), P(None, "tp"), P("tp", None)
    return jax.shard_map(
        step,
        mesh=mesh,
        in_specs=(tokens, tokens, P("dp", "tp"), P("dp", "tp"), columns, columns, rows),
        out_specs=(tokens, P("dp", "tp"), P("dp", "tp"), P(("dp", "tp"), None)),
        check_vma=False,
    )
```

```python
import functools

import jax
import jax.numpy as jnp
from jax import lax
from jax.experimental import pallas as pl
from jax.experimental.pallas import tpu as pltpu
from jax.sharding import PartitionSpec as P

ROWS, D, F = 2048, 2304, 1152
R = 256
H = R // 2
Q = D // 2
NK = ROWS // R
NT = (((1,), (1,)), ((), ()))
TN = (((0,), (0,)), ((), ()))
MESH = pl.DeviceIdType.MESH
f32, bf16 = jnp.float32, jnp.bfloat16
C1 = 0.7978845608028654
C3 = 0.044715

S_X, S_Y, S_END = 14, 23, 32
AT = {
    2: (3, 4, 9, 9, 12, 17, 19, 19),
    3: (5, 6, 13, 14, 19, 20, 22, 24),
    4: (8, 15, 16, 18, 25, 25, 28, 29),
    5: (13, 24, 25, 26, 29, 30, 32, 33),
}
EARLY, EARLY_CHUNKS = 32, 6
D_TILES = ((0, 256), (256, 512), (512, 768), (768, 1024), (1024, 1152))


def act_back(g, u, d):
    g2 = g * g
    t = jnp.tanh(g * (C1 + (C1 * C3) * g2))
    cdf = 0.5 + 0.5 * t
    gelu = g * cdf
    slope = cdf + (0.5 * g) * (1.0 - t * t) * (C1 + (3 * C1 * C3) * g2)
    return gelu * u, d * u * slope, d * gelu


def main_kernel(
    x, dy, gate, up, wg, wu, wd,
    dx, wgu, wdo,
    gu, hid, cur0, cur1, dyv, gv, uv, xyv, own, psend, pin, r1, r2, kept1, kept2,
    ssem, rsem, wsem, isem, xsem,
):
    me = lax.axis_index("tp")
    xb, yb, cb = lax.div(me, 4), lax.rem(lax.div(me, 2), 2), lax.rem(me, 2)
    mate = me + 1 - 2 * cb

    def wd_in(i):
        rows = pl.ds((0, 512)[i], (512, 640)[i])
        return pltpu.make_async_copy(wd.at[rows], wdo.at[rows], wsem.at[0, i])

    def wgu_in(i):
        rows = pl.ds(768 * i, 768)
        return [
            pltpu.make_async_copy(w.at[rows], wgu.at[rows, pl.ds(F * q, F)], wsem.at[1 + q, i])
            for q, w in enumerate((wg, wu))
        ]

    def half_rows(k, half):
        at = k * R + H * (half * cb + (1 - half) * (1 - cb))
        return pl.ds(pl.multiple_of(at, H), H)

    def rows_in(k):
        slot = lax.rem(k, 2)
        return [
            pltpu.make_async_copy(
                src.at[half_rows(k, half)],
                dst.at[slot, pl.ds(H * half, H)],
                isem.at[i, half, slot],
            )
            for i, (src, dst) in enumerate(((dy, dyv), (gate, gv), (up, uv)))
            for half in range(2)
        ]

    def tile_in(src, j, q):
        slot = lax.rem(q, 2)
        columns = pl.ds(pl.multiple_of(j * 256, 256), 256)
        return pltpu.make_async_copy(src.at[:, columns], xyv.at[slot], xsem.at[slot])

    for copy in rows_in(0):
        copy.start()
    for i in range(2):
        wd_in(i).start()

    barrier = pltpu.get_barrier_semaphore()
    for other in (mate, me + 2 * (1 - 2 * yb), me + 4 * (1 - 2 * xb)):
        pl.semaphore_signal(barrier, inc=1, device_id={"tp": other}, device_id_type=MESH)

    x_pair, y_pair = (xb, me + 4 * (1 - 2 * xb)), (yb, me + 2 * (1 - 2 * yb))
    LINKS = ((x_pair, y_pair), (y_pair, x_pair))

    def remote(i, k, p, src, dst, to):
        return pltpu.make_async_remote_copy(
            src_ref=src, dst_ref=dst, send_sem=ssem.at[i, p, k], recv_sem=rsem.at[i, p, k],
            device_id={"tp": to}, device_id_type=MESH,
        )

    def sl(start, size, unit):
        return pl.ds(pl.multiple_of(start, unit), size)

    keep1, give1, keep2, give2 = ([f(p) for p in range(2)] for f in (
        lambda p: 64 * LINKS[p][0][0],
        lambda p: 64 - 64 * LINKS[p][0][0],
        lambda p: 32 * LINKS[p][1][0],
        lambda p: 32 - 32 * LINKS[p][1][0],
    ))

    def mate_term(k, p):
        return remote(0, k, p, psend.at[p], pin.at[p, k], mate)

    def half_sum(k, p):
        return remote(1, k, p, pin.at[p, k, sl(give1[p], 64, 64)], r1.at[p, k], LINKS[p][0][1])

    def quarter_sum(k, p):
        return remote(2, k, p, r1.at[p, k, sl(give2[p], 32, 32)], r2.at[p, k], LINKS[p][1][1])

    def dx_copy(i, k, p, to, row, size):
        ref = dx.at[sl(k * R + (cb * H + row), size, 32), p * Q:(p + 1) * Q]
        return remote(i, k, p, ref, ref, to)

    def final(k, p, to):
        i, device = {
            "second": (3, LINKS[p][1][1]), "first": (4, LINKS[p][0][1]), "mate": (6, mate)
        }[to]
        return dx_copy(i, k, p, device, keep1[p] + keep2[p], 32)

    def forward(k, p, to):
        i, device = {"first": (5, LINKS[p][0][1]), "mate": (7, mate)}[to]
        return dx_copy(i, k, p, device, keep1[p] + give2[p], 32)

    def last(k, p):
        return dx_copy(8, k, p, mate, give1[p], 64)

    def ring(k):
        return lax.rem(k, 4)

    def stage1(k, p):
        mate_term(k, p).wait_recv()

        def total(r):
            mine = own[sl(r, 16, 16), p * Q:(p + 1) * Q]
            return mine + pin[p, k, sl(r, 16, 16), :].astype(f32)

        for i in range(4):
            r = give1[p] + 16 * i
            pin[p, k, sl(r, 16, 16), :] = total(r).astype(bf16)
        half_sum(k, p).start()
        for i in range(4):
            kept1[p, ring(k), 16 * i:16 * i + 16, :] = total(keep1[p] + 16 * i)

    def stage2(k, p):
        half_sum(k, p).wait_recv()

        def total(r):
            mine = kept1[p, ring(k), sl(r, 16, 16), :]
            return mine + r1[p, k, sl(r, 16, 16), :].astype(f32)

        for i in range(2):
            r = give2[p] + 16 * i
            r1[p, k, sl(r, 16, 16), :] = total(r).astype(bf16)
        quarter_sum(k, p).start()
        for i in range(2):
            kept2[p, ring(k), 16 * i:16 * i + 16, :] = total(keep2[p] + 16 * i)

    def stage3(k, p):
        quarter_sum(k, p).wait_recv()
        base = k * R + (cb * H + keep1[p] + keep2[p])
        for i in range(2):
            part = slice(16 * i, 16 * i + 16)
            t = kept2[p, ring(k), part, :] + r2[p, k, part, :].astype(f32)
            dx[sl(base + 16 * i, 16, 16), p * Q:(p + 1) * Q] = t.astype(bf16)
        for to in ("second", "first", "mate"):
            final(k, p, to).start()

    def stage4(k, p):
        final(k, p, "second").wait_recv()
        for to in ("first", "mate"):
            forward(k, p, to).start()

    def stage5(k, p):
        final(k, p, "first").wait_recv()
        forward(k, p, "first").wait_recv()
        last(k, p).start()

    STAGES = {2: stage2, 3: stage3, 4: stage4, 5: stage5}

    def run_step(step):
        for stage in (5, 4, 3, 2):
            for k in range(NK):
                if AT[stage][k] == step:
                    STAGES[stage](k, 0)
                    STAGES[stage](k, 1)

    def serve(i, first, stride, turns):
        for v in range(turns):
            if any(first + stride * v in at for at in AT.values()):
                pl.when(i == v)(functools.partial(run_step, first + stride * v))

    def back_tile(k, cur, n0, n1):
        slot = lax.rem(k, 2)
        d = lax.dot_general(dyv[slot], wdo[n0:n1, :], NT, preferred_element_type=f32)
        grads = act_back(gv[slot, :, n0:n1].astype(f32), uv[slot, :, n0:n1].astype(f32), d)
        h, dg, du = (g.astype(bf16) for g in grads)
        cur[:, n0:n1] = dg
        cur[:, F + n0:F + n1] = du
        for half in range(2):
            rows, part = half_rows(k, half), slice(H * half, H * half + H)
            gu[rows, n0:n1] = dg[part]
            gu[rows, F + n0:F + n1] = du[part]
            hid[rows, n0:n1] = h[part]

    def term_tile(cur, n0):
        t = lax.dot_general(
            cur[...], wgu[n0:n0 + 768, :], NT, preferred_element_type=f32
        )
        own[:, n0:n0 + 768] = t[H:]
        for p, q0, q1 in ((0, n0, min(n0 + 768, Q)), (1, max(n0, Q), n0 + 768)):
            if q0 < q1:
                psend[p, :, q0 - p * Q:q1 - p * Q] = t[:H, q0 - n0:q1 - n0].astype(bf16)

    def send_term(k):
        for p in range(2):
            mate_term(k, p).start()

    def chunk_sum(k):
        stage1(k, 0)
        stage1(k, 1)

    def chunk_step(m, k, first, cur, ahead, start_rows):
        for p in range(2):
            mate_term(k - 1, p).wait_send()
        for copy in rows_in(k + 1):
            copy.wait()
        start_rows()
        for n0 in range(0, D, 768):
            term_tile(cur, n0)
        send_term(k)
        serve(m, first, 4, 3)
        for n0, n1 in D_TILES:
            back_tile(k + 1, ahead, n0, n1)
        chunk_sum(k)
        serve(m, first + 1, 4, 3)

    for copy in rows_in(0):
        copy.wait()
    for i in range(3):
        for copy in wgu_in(i):
            copy.start()
    wd_in(0).wait()
    for n0, n1 in D_TILES:
        if n0 == 512:
            wd_in(1).wait()
        back_tile(0, cur0, n0, n1)
    for copy in rows_in(1):
        copy.start()
    for i in range(3):
        for copy in wgu_in(i):
            copy.wait()
        term_tile(cur0, 768 * i)
    pl.semaphore_wait(barrier, 3)
    send_term(0)
    for copy in rows_in(1):
        copy.wait()
    for copy in rows_in(2):
        copy.start()
    for n0, n1 in D_TILES:
        back_tile(1, cur1, n0, n1)
    chunk_sum(0)

    def two_chunks(m, z):
        def next_rows(k):
            for copy in rows_in(k):
                copy.start()

        chunk_step(m, 2 * m + 1, 1, cur1, cur0, lambda: next_rows(2 * m + 3))
        chunk_step(
            m, 2 * m + 2, 3, cur0, cur1,
            lambda: pl.when(m < 2)(lambda: next_rows(2 * m + 4)),
        )
        return z

    lax.fori_loop(0, NK // 2 - 1, two_chunks, 0)
    tile_in(x, 0, 0).start()
    for p in range(2):
        mate_term(NK - 2, p).wait_send()
    for n0 in range(0, D, 768):
        term_tile(cur1, n0)
    send_term(NK - 1)
    run_step(2 * NK - 3)

    def x_tile(j, z):
        slot = lax.rem(j, 2)

        @pl.when(j + 1 < 9)
        def _():
            tile_in(x, j + 1, j + 1).start()

        @pl.when(j + 1 == 9)
        def _():
            tile_in(dy, 0, 9).start()

        tile_in(x, j, j).wait()
        rows = sl(j * 256, 256, 256)
        for n0 in range(0, D, 768):
            wgu[rows, n0:n0 + 768] = lax.dot_general(
                xyv[slot], gu[:, n0:n0 + 768], TN, preferred_element_type=f32
            ).astype(bf16)

        @pl.when(j == 0)
        def _():
            chunk_sum(NK - 1)

        serve(j, S_X, 1, 9)
        return z

    lax.fori_loop(0, 9, x_tile, 0)

    def y_tile(j, z):
        slot = lax.rem(j + 1, 2)

        @pl.when(j + 1 < 9)
        def _():
            tile_in(dy, j + 1, j + 10).start()

        tile_in(dy, j, j + 9).wait()
        wdo[:, sl(j * 256, 256, 256)] = lax.dot_general(
            hid[...], xyv[slot], TN, preferred_element_type=f32
        ).astype(bf16)
        serve(j, S_Y, 1, 9)
        return z

    lax.fori_loop(0, 9, y_tile, 0)
    def finish(k):
        for p in range(2):
            half_sum(k, p).wait_send()
            quarter_sum(k, p).wait_send()
            for to in ("second", "first", "mate"):
                final(k, p, to).wait_send()
            for to in ("first", "mate"):
                forward(k, p, to).wait_send()
            last(k, p).wait_send()
            final(k, p, "mate").wait_recv()
            forward(k, p, "mate").wait_recv()
            last(k, p).wait_recv()

    for p in range(2):
        mate_term(NK - 1, p).wait_send()
    for step in range(S_END, max(*AT[5], EARLY) + 1):
        run_step(step)
        if step == EARLY:
            for k in range(EARLY_CHUNKS):
                finish(k)
    for k in range(EARLY_CHUNKS, NK):
        finish(k)


def write_kernel(dx, wgu, wdo, dx_o, wg_o, wu_o, wd_o, sem):
    copies = []
    for at in range(4):
        for src, dst in (
            (dx, dx_o), (wgu.at[:, pl.ds(0, F)], wg_o), (wgu.at[:, pl.ds(F, F)], wu_o), (wdo, wd_o)
        ):
            size = src.shape[0] // 4
            rows = pl.ds(at * size, size)
            copies.append(
                pltpu.make_async_copy(src.at[rows], dst.at[rows], sem.at[len(copies)])
            )
    for copy in copies:
        copy.start()
    for copy in copies:
        copy.wait()


def solution(mesh):
    hbm = pl.BlockSpec(memory_space=pltpu.HBM)
    vmem = pl.BlockSpec(memory_space=pltpu.VMEM)

    def step(x, dy, gate, up, wg, wu, wd):
        results = pl.pallas_call(
            main_kernel,
            name="mlp_back",
            out_shape=(
                pltpu.VMEM((ROWS, D), bf16),
                pltpu.VMEM((D, D), bf16),
                pltpu.VMEM((F, D), bf16),
            ),
            in_specs=[hbm] * 7,
            out_specs=(vmem,) * 3,
            scratch_shapes=[
                pltpu.VMEM((ROWS, D), bf16),
                pltpu.VMEM((ROWS, F), bf16),
                pltpu.VMEM((R, D), bf16),
                pltpu.VMEM((R, D), bf16),
                pltpu.VMEM((2, R, D), bf16),
                pltpu.VMEM((2, R, F), bf16),
                pltpu.VMEM((2, R, F), bf16),
                pltpu.VMEM((2, ROWS, 256), bf16),
                pltpu.VMEM((H, D), f32),
                pltpu.VMEM((2, H, Q), bf16),
                pltpu.VMEM((2, NK, H, Q), bf16),
                pltpu.VMEM((2, NK, 64, Q), bf16),
                pltpu.VMEM((2, NK, 32, Q), bf16),
                pltpu.VMEM((2, 4, 64, Q), f32),
                pltpu.VMEM((2, 4, 32, Q), f32),
                pltpu.SemaphoreType.DMA((9, 2, NK)),
                pltpu.SemaphoreType.DMA((9, 2, NK)),
                pltpu.SemaphoreType.DMA((3, 3)),
                pltpu.SemaphoreType.DMA((3, 2, 2)),
                pltpu.SemaphoreType.DMA((2,)),
            ],
            compiler_params=pltpu.CompilerParams(
                collective_id=0, has_side_effects=True, vmem_limit_bytes=38 * 2**20
            ),
            cost_estimate=pl.CostEstimate(
                flops=12 * ROWS * D * F, bytes_accessed=80 * 2**20, transcendentals=ROWS * F
            ),
        )(x, dy, gate, up, wg, wu, wd)
        return pl.pallas_call(
            write_kernel,
            name="write_out",
            out_shape=(
                jax.ShapeDtypeStruct((ROWS, D), bf16),
                jax.ShapeDtypeStruct((D, F), bf16),
                jax.ShapeDtypeStruct((D, F), bf16),
                jax.ShapeDtypeStruct((F, D), bf16),
            ),
            in_specs=[vmem] * 3,
            out_specs=(hbm,) * 4,
            scratch_shapes=[pltpu.SemaphoreType.DMA((16,))],
            compiler_params=pltpu.CompilerParams(vmem_limit_bytes=8 * 2**20),
        )(*results)

    tokens, columns, rows = P("dp", None), P(None, "tp"), P("tp", None)
    return jax.shard_map(
        step,
        mesh=mesh,
        in_specs=(tokens, tokens, P("dp", "tp"), P("dp", "tp"), columns, columns, rows),
        out_specs=(tokens, P("dp", "tp"), P("dp", "tp"), P(("dp", "tp"), None)),
        check_vma=False,
    )
```
